32 devices in a mesh: section: 8 (over z, y), dp: 4 (over x, core).
Axes of the slice: x: 2, y: 2, z: 4, core: 2. Of those that a mesh axis runs over, the one named last changes fastest.
Arguments:
- vit_weight: bfloat16 [8, 1280, 1280], P('section', 'dp'), may hold values from -0.078125 to 0.078125
- t5_weight: bfloat16 [8, 2048, 2048], P('section', 'dp'), may hold values from -0.0625 to 0.0625
- vit_saved: bfloat16 [8, 4, 128, 1280], P('section', None, 'dp'), may hold values from -6 to 6
- t5_saved: bfloat16 [8, 4, 128, 2048], P('section', None, 'dp'), may hold values from -6 to 6
- vit_top_grad: bfloat16 [4, 128, 1280], P(None, 'dp'), may hold values from -6 to 6
- t5_top_grad: bfloat16 [4, 128, 2048], P(None, 'dp'), may hold values from -6 to 6
Outputs:
- vit_input_grads: bfloat16 [8, 4, 128, 1280], P('section', None, 'dp')
- t5_input_grads: bfloat16 [8, 4, 128, 2048], P('section', None, 'dp')
- vit_weight_grads: float32 [8, 1280, 1280], P('section', 'dp')
- t5_weight_grads: float32 [8, 2048, 2048], P('section', 'dp')
The draws below stay inside these ranges and needn't reach their ends.
All inputs are finite; a program needn't handle non-finite values.
Results may differ from the reference program's by a relative error of at most 0.02.
Values may be sent and summed in bfloat16 or wider, within the bound.
A program may use at most 128 MiB of HBM per device.

```python
import jax
import jax.numpy as jnp
from jax import lax

DV = 1280
DT = 2048
TOK = 32
MB = 4
LAYERS = 8
TOKENS = 128
N_DP = 4


def spiked(entries, own_key, source, target, blocks, factor):
    owner, partner = [(jnp.arange(entries.shape[axis_at]) // (entries.shape[axis_at] // blocks)).reshape([-1 if axis == axis_at else 1 for axis in range(entries.ndim)]) for axis_at in (source, target)]
    chosen = jax.random.permutation(own_key, blocks)[partner]
    strong = (owner == chosen) | (owner == (partner + blocks // 2) % blocks)
    return jnp.where(strong, factor * entries, entries)


def level_of(own_key, shape, pieces, low, high):
    def one(dim, blocks):
        heights = jax.random.uniform(jax.random.fold_in(jax.random.fold_in(own_key, 6), dim), (blocks,), jnp.float32, low / len(pieces), high / len(pieces))
        return jnp.repeat(jnp.exp(heights), shape[dim] // blocks).reshape((-1,) + (1,) * (len(shape) - dim - 1))

    loudness = one(*pieces[0])
    for cut in pieces[1:]:
        loudness = loudness * one(*cut)
    return loudness


def normal_values(rng, shape, width, most, split=(), kind=jnp.bfloat16):
    drawn = jax.random.normal(rng, shape, jnp.float32) * width
    if len(split) > 0:
        drawn = level_of(rng, shape, split, -0.22, 0.18) * drawn
    return jnp.clip(drawn, min=-most, max=most).astype(kind)


def gaussian_with(own_key, dims, scale, bound, split, heavy, dtype=jnp.bfloat16):
    values = scale * jax.random.normal(own_key, dims, jnp.float32)
    if split:
        values = values * level_of(own_key, dims, split, -0.22, 0.18)
    return jnp.clip(spiked(values, jax.random.fold_in(own_key, 3), *heavy), -bound, bound).astype(dtype)


def setup_inputs(seed: int = 0) -> dict:
    keys = jax.random.split(jax.random.key(seed), 7)
    return {
        "vit_weight": normal_values(keys[0], (LAYERS, DV, DV), (4 * DV) ** -0.5, 0.078125, ((0, 8), (1, 4))),
        "t5_weight": normal_values(keys[1], (LAYERS, DT, DT), (4 * DT) ** -0.5, 0.0625, ((0, 8), (1, 4))),
        "vit_saved": gaussian_with(keys[2], (LAYERS, MB, TOKENS, DV), 1.0, 6.0, ((0, 8), (2, 4)), (2, 3, 4, 2.0)),
        "t5_saved": gaussian_with(keys[3], (LAYERS, MB, TOKENS, DT), 1.0, 6.0, ((0, 8), (2, 4)), (2, 3, 4, 2.0)),
        "vit_top_grad": normal_values(keys[4], (MB, TOKENS, DV), 1.0, 6.0, ((1, 4),)),
        "t5_top_grad": normal_values(keys[5], (MB, TOKENS, DT), 1.0, 6.0, ((1, 4),)),
    }


root_half = 0.7071067811865476
inv_root_tau = 0.3989422804014327


def gelu_slope(preact):
    cumulative = 0.5 * (1.0 + lax.erf(preact * root_half))
    density = jnp.exp(-0.5 * preact * preact) * inv_root_tau
    return cumulative + preact * density


def layer_back(grad_above, saved_input, weight):
    preact = jnp.dot(saved_input, weight, preferred_element_type=jnp.float32)
    upper = grad_above.astype(jnp.float32)
    local_grad = (upper * gelu_slope(preact)).astype(jnp.bfloat16)
    through = jnp.dot(local_grad, weight.T, preferred_element_type=jnp.float32)
    return (upper + through).astype(jnp.bfloat16), local_grad


def run_branch(weights, saved, top_grad):
    layer_count = weights.shape[0]
    features = top_grad.shape[2]
    grad_above = top_grad.reshape(MB * TOKENS, features)
    input_grads = [None] * layer_count
    weight_grads = [None] * layer_count
    for layer_index in reversed(range(layer_count)):
        saved_input = saved[layer_index].reshape(MB * TOKENS, features)
        grad_below, local_grad = layer_back(grad_above, saved_input, weights[layer_index])
        grouped_input = saved_input.astype(jnp.float32).reshape(MB, N_DP, TOK, features)
        grouped_local = local_grad.astype(jnp.float32).reshape(MB, N_DP, TOK, features)
        partial_value = jnp.einsum("mpti,mptj->pij", grouped_input, grouped_local) * (1.0 / (MB * TOK))
        rounded = lax.optimization_barrier(partial_value.astype(jnp.bfloat16))
        weight_grads[layer_index] = jnp.sum(rounded.astype(jnp.float32), axis=0)
        input_grads[layer_index] = grad_below.reshape(MB, TOKENS, features)
        grad_above = grad_below
    return jnp.stack(input_grads), jnp.stack(weight_grads)


def reference(vit_weight, t5_weight, vit_saved, t5_saved, vit_top_grad, t5_top_grad):
    vit_grads, vit_wgrads = run_branch(vit_weight, vit_saved, vit_top_grad)
    t5_grads, t5_wgrads = run_branch(t5_weight, t5_saved, t5_top_grad)
    return (vit_grads, t5_grads, vit_wgrads, t5_wgrads)
```

```python
import jax
import jax.numpy as jnp
from jax import lax
from jax.sharding import PartitionSpec as P

root_half = 0.7071067811865476
inv_root_tau = 0.3989422804014327


def shifted(block, axis, distance):
    devices = range(lax.axis_size(axis))
    route = [(i - distance, i) for i in devices if i - distance in devices]
    return lax.ppermute(block, axis, route)


def gelu_slope(preact):
    cumulative = 0.5 * (1.0 + lax.erf(preact * root_half))
    density = jnp.exp(-0.5 * preact * preact) * inv_root_tau
    return cumulative + preact * density


def slopes(saved, weight):
    flat = saved.reshape(-1, saved.shape[-1])
    return gelu_slope(jnp.dot(flat, weight, preferred_element_type=jnp.float32)).reshape(saved.shape)


def token_columns(saved):
    flat = saved.reshape(-1, saved.shape[-1])
    parts = lax.axis_size("dp")
    split = flat.reshape(flat.shape[0], parts, -1).transpose(1, 0, 2)
    return lax.all_to_all(split, "dp", 0, 0, tiled=True)


def weight_rows(columns, locals_all, scale):
    total = jnp.zeros((columns.shape[2], locals_all.shape[2]), jnp.float32)
    for group in range(columns.shape[0]):
        term = lax.dot_general(
            columns[group], locals_all[group], (((0,), (0,)), ((), ())),
            preferred_element_type=jnp.float32,
        )
        total = total + (term * scale).astype(jnp.bfloat16).astype(jnp.float32)
    return total


def shards(vit_weight, t5_weight, vit_saved, t5_saved, vit_top_grad, t5_top_grad):
    section_count = lax.axis_size("section")
    section_index = lax.axis_index("section")
    is_last = section_index == section_count - 1
    depth = section_count - 1 - section_index
    weights = [lax.all_gather(w[0], "dp", axis=0, tiled=True) for w in (t5_weight, vit_weight)]
    saved = [t5_saved[0], vit_saved[0]]
    tops = [t5_top_grad, vit_top_grad]
    columns = [token_columns(s) for s in saved]
    slope = [slopes(s, w) for s, w in zip(saved, weights)]
    micro_count, token_count = saved[0].shape[:2]
    scale = 1.0 / (micro_count * token_count)

    def tick(index, state):
        micro = index - depth
        active = jnp.logical_and(micro >= 0, micro < micro_count)
        slot = jnp.clip(micro, 0, micro_count - 1)

        def advance(operands):
            result = []
            for (received, grads, locals_now), w, top, sl in zip(operands, weights, tops, slope):
                above = jnp.where(is_last, top[slot], received)
                upper = above.astype(jnp.float32)
                local = (upper * sl[slot]).astype(jnp.bfloat16)
                through = lax.dot_general(
                    local, w, (((1,), (1,)), ((), ())), preferred_element_type=jnp.float32
                )
                below = (upper + through).astype(jnp.bfloat16)
                result.append((
                    below,
                    lax.dynamic_update_index_in_dim(grads, below, slot, 0),
                    lax.dynamic_update_index_in_dim(locals_now, local, slot, 0),
                ))
            return tuple(result)

        state = lax.cond(active, advance, lambda operands: operands, state)
        return tuple((shifted(a, "section", -1), b, c) for a, b, c in state)

    start = tuple(
        (jnp.zeros_like(top[0]), jnp.zeros_like(s), jnp.zeros_like(s)) for top, s in zip(tops, saved)
    )
    state = lax.fori_loop(0, section_count + micro_count - 1, tick, start)
    sums = []
    for (_, _, locals_now), cols in zip(state, columns):
        flat = locals_now.reshape(-1, locals_now.shape[-1])
        everyone = lax.all_gather(flat, "dp", axis=0, tiled=False)
        sums.append(weight_rows(cols, everyone, scale))
    return (state[1][1][None], state[0][1][None], sums[1][None], sums[0][None])


def solution(mesh):
    placed = (
        P("section", "dp", None),
        P("section", "dp", None),
        P("section", None, "dp", None),
        P("section", None, "dp", None),
        P(None, "dp", None),
        P(None, "dp", None),
    )
    return jax.shard_map(
        shards,
        mesh=mesh,
        in_specs=placed,
        out_specs=(
            P("section", None, "dp", None),
            P("section", None, "dp", None),
            P("section", "dp", None),
            P("section", "dp", None),
        ),
        check_vma=False,
    )
```

```python
import functools

import jax
import jax.numpy as jnp
from jax import lax
from jax.experimental import pallas as pl
from jax.experimental.pallas import tpu as pltpu
from jax.sharding import PartitionSpec as P

root_half = 0.7071067811865476
inv_root_tau = 0.3989422804014327
MESH = pl.DeviceIdType.MESH


def gelu_slope(preact):
    cumulative = 0.5 * (1.0 + lax.erf(preact * root_half))
    density = jnp.exp(-0.5 * preact * preact) * inv_root_tau
    return cumulative + preact * density


class Branch:
    def __init__(self, ins, outs, scratch):
        self.weight, self.saved, self.top = ins
        self.out, self.columns, self.local = outs
        (
            self.above,
            self.below,
            self.mine,
            self.pair_out,
            self.pair_in,
            self.chip_in,
            self.slope,
            self.saved_sem,
            self.top_sem,
            self.pair_sem,
            self.chip_sem,
            self.near_sem,
            self.far_sem,
            self.hop_sem,
            self.out_sem,
        ) = scratch


BRANCH_SCRATCH = 15


def kernel(sections, parts, micros, *refs):
    ins, outs, scratch = refs[:6], refs[6:12], refs[12:]
    branches = [
        Branch(ins[3 * b : 3 * b + 3], outs[3 * b : 3 * b + 3],
               scratch[BRANCH_SCRATCH * b : BRANCH_SCRATCH * (b + 1)])
        for b in range(2)
    ]
    section = lax.axis_index("section")
    me = lax.axis_index("dp")
    chips = parts // 2
    chip, core = me // 2, me % 2
    partner = chip * 2 + 1 - core
    is_last = section == sections - 1
    is_first = section == 0

    def ahead(k):
        return lax.rem(chip + k, chips) * 2 + core

    def behind(k):
        return lax.rem(chip + chips - k, chips) * 2 + core

    def other(group):
        return group + 1 - 2 * core

    def copy(src, dst, sems, index, where, part):
        return pltpu.make_async_remote_copy(
            src_ref=src, dst_ref=dst, send_sem=sems.at[(0, *index)], recv_sem=sems.at[(1, *index)],
            device_id=(where, part), device_id_type=MESH,
        )

    barrier = pltpu.get_barrier_semaphore()
    for k in range(1, parts):
        pl.semaphore_signal(barrier, inc=1, device_id=(section, lax.rem(me + k, parts)), device_id_type=MESH)

    @pl.when(section > 0)
    def _():
        pl.semaphore_signal(barrier, inc=1, device_id=(section - 1, me), device_id_type=MESH)

    @pl.when(section < sections - 1)
    def _():
        pl.semaphore_signal(barrier, inc=1, device_id=(section + 1, me), device_id_type=MESH)

    neighbours = lax.min(section, 1) + lax.min(sections - 1 - section, 1)
    pl.semaphore_wait(barrier, parts - 1 + neighbours)

    def saved_copy(br, m, k):
        to = lax.rem(me + k, parts)
        return copy(br.saved.at[to, m], br.columns.at[m, me], br.saved_sem, (m, k - 1), section, to)

    def top_copy(br, m, k):
        to = lax.rem(me + k, parts)
        return copy(br.top.at[to, m], br.above.at[m, me], br.top_sem, (m, k - 1), section, to)

    def pair_copy(br, m):
        return copy(br.pair_out.at[m], br.pair_in.at[m], br.pair_sem, (m,), section, partner)

    def chip_copy(br, m, k):
        return copy(br.mine.at[m, k], br.chip_in.at[m, k - 1], br.chip_sem, (m, k - 1), section, ahead(k))

    def near_copy(br, m, k):
        group = behind(k)
        return copy(br.local.at[m, group], br.local.at[m, group], br.near_sem, (m, k), section, partner)

    def far_copy(br, m, k):
        return copy(br.local.at[m, me], br.local.at[m, me], br.far_sem, (m, k - 1), section, ahead(k))

    def hop_copy(br, m):
        return copy(br.below.at[m], br.above.at[m], br.hop_sem, (m,), lax.max(section - 1, 0), me)

    def out_copy(br, m, k):
        to = lax.rem(me + k, parts)
        return copy(br.below.at[m, to], br.out.at[me, m], br.out_sem, (m, k - 1), section, to)

    def rows(block):
        return block.reshape(-1, block.shape[-1])

    def send_inputs(m):
        for br in branches:
            for k in range(1, parts):
                saved_copy(br, m, k).start()

            @pl.when(is_last)
            def _():
                for k in range(1, parts):
                    top_copy(br, m, k).start()

    def partial(m):
        for br in branches:
            br.columns[m, me] = br.saved[me, m]
            for k in range(1, parts):
                saved_copy(br, m, k).wait_recv()
            tokens = rows(br.columns[m])
            for k in range(chips):
                group = ahead(k)
                br.pair_out[m, k] = jnp.dot(
                    tokens, br.weight[other(group)], preferred_element_type=jnp.float32
                ).astype(jnp.bfloat16)
            pair_copy(br, m).start()
            for k in range(chips):
                br.mine[m, k] = jnp.dot(
                    tokens, br.weight[ahead(k)], preferred_element_type=jnp.float32
                ).astype(jnp.bfloat16)

    def pair_sum(m):
        for br in branches:
            pair_copy(br, m).wait_recv()
            for k in range(1, chips):
                both = br.mine[m, k].astype(jnp.float32) + br.pair_in[m, k].astype(jnp.float32)
                br.mine[m, k] = both.astype(jnp.bfloat16)
                chip_copy(br, m, k).start()

    def find_slope(m):
        for br in branches:
            total = br.mine[m, 0].astype(jnp.float32) + br.pair_in[m, 0].astype(jnp.float32)
            for k in range(1, chips):
                chip_copy(br, m, k).wait_recv()
                total = total + br.chip_in[m, k - 1].astype(jnp.float32)
            br.slope[m] = gelu_slope(total)

    def chain(m):
        for br in branches:
            @pl.when(is_last)
            def _():
                br.above[m, me] = br.top[me, m]
                for k in range(1, parts):
                    top_copy(br, m, k).wait_recv()

            @pl.when(jnp.logical_not(is_last))
            def _():
                hop_copy(br, m).wait_recv()

            br.local[m, me] = (rows(br.above[m]).astype(jnp.float32) * br.slope[m]).astype(jnp.bfloat16)
            for k in range(1, chips):
                far_copy(br, m, k).start()
            near_copy(br, m, 0).start()
        for br in branches:
            def through(group):
                return lax.dot_general(
                    br.local[m, group], br.weight[group], (((1,), (1,)), ((), ())),
                    preferred_element_type=jnp.float32,
                )

            total = rows(br.above[m]).astype(jnp.float32) + through(me)
            near_copy(br, m, 0).wait_recv()
            total = total + through(partner)
            for k in range(1, chips):
                far_copy(br, m, k).wait_recv()
                near_copy(br, m, k).start()
                total = total + through(behind(k))
            for k in range(1, chips):
                near_copy(br, m, k).wait_recv()
                total = total + through(other(behind(k)))
            br.below[m] = total.astype(jnp.bfloat16).reshape(br.below.shape[1:])

            @pl.when(jnp.logical_not(is_first))
            def _():
                hop_copy(br, m).start()

            br.out[me, m] = br.below[m, me]
            for k in range(1, parts):
                out_copy(br, m, k).start()

    def loop(body):
        pl.loop(0, micros)(body)

    loop(send_inputs)
    loop(partial)
    loop(pair_sum)

    @pl.loop(0, micros)
    def _(m):
        find_slope(m)
        chain(m)

    @pl.loop(0, micros)
    def _(m):
        for br in branches:
            for k in range(1, parts):
                saved_copy(br, m, k).wait_send()
                out_copy(br, m, k).wait_send()
                out_copy(br, m, k).wait_recv()

            @pl.when(is_last)
            def _():
                for k in range(1, parts):
                    top_copy(br, m, k).wait_send()

            @pl.when(jnp.logical_not(is_first))
            def _():
                hop_copy(br, m).wait_send()

            pair_copy(br, m).wait_send()
            near_copy(br, m, 0).wait_send()
            for k in range(1, chips):
                chip_copy(br, m, k).wait_send()
                far_copy(br, m, k).wait_send()
                near_copy(br, m, k).wait_send()


def branch_call(sections, weights, saveds, tops):
    operands, outs, scratch = [], [], []
    for weight, saved, top in zip(weights, saveds, tops):
        parts, rows, _ = weight.shape
        micros, tokens = saved.shape[1:3]
        chips = parts // 2
        everyone = parts * tokens
        operands += [weight, saved, top]
        outs += [
            jax.ShapeDtypeStruct((parts, micros, tokens, rows), jnp.bfloat16),
            jax.ShapeDtypeStruct((micros, parts, tokens, rows), jnp.bfloat16),
            jax.ShapeDtypeStruct((micros, parts, everyone, rows), jnp.bfloat16),
        ]
        dma = pltpu.SemaphoreType.DMA
        scratch += [
            pltpu.VMEM((micros, parts, tokens, rows), jnp.bfloat16),
            pltpu.VMEM((micros, parts, tokens, rows), jnp.bfloat16),
            pltpu.VMEM((micros, chips, everyone, rows), jnp.bfloat16),
            pltpu.VMEM((micros, chips, everyone, rows), jnp.bfloat16),
            pltpu.VMEM((micros, chips, everyone, rows), jnp.bfloat16),
            pltpu.VMEM((micros, max(chips - 1, 1), everyone, rows), jnp.bfloat16),
            pltpu.VMEM((micros, everyone, rows), jnp.float32),
            dma((2, micros, parts - 1)),
            dma((2, micros, parts - 1)),
            dma((2, micros)),
            dma((2, micros, max(chips - 1, 1))),
            dma((2, micros, chips)),
            dma((2, micros, max(chips - 1, 1))),
            dma((2, micros)),
            dma((2, micros, parts - 1)),
        ]
    vmem = pl.BlockSpec(memory_space=pltpu.VMEM)
    return pl.pallas_call(
        functools.partial(kernel, sections, parts, micros),
        out_shape=outs,
        in_specs=[vmem] * len(operands),
        out_specs=[vmem] * len(outs),
        scratch_shapes=scratch,
        compiler_params=pltpu.CompilerParams(
            collective_id=0, has_side_effects=True, vmem_limit_bytes=60 * 1024 * 1024
        ),
    )(*operands)


def feature_groups(block, parts):
    return jnp.moveaxis(block.reshape(*block.shape[:-1], parts, -1), -2, 0)


def weight_rows(columns, locals_all, scale):
    micros, parts, tokens, rows = columns.shape
    columns = columns.astype(jnp.bfloat16)
    by_group = locals_all.reshape(micros, parts, parts, tokens, rows)
    total = None
    for group in range(parts):
        left = columns[:, group].reshape(-1, rows)
        right = by_group[:, :, group].transpose(0, 2, 1, 3).reshape(micros * tokens, -1)
        term = lax.dot_general(
            left, right, (((0,), (0,)), ((), ())), preferred_element_type=jnp.float32
        )
        term = (term * scale).astype(jnp.bfloat16).astype(jnp.float32)
        total = term if total is None else total + term
    return total


def shards(vit_weight, t5_weight, vit_saved, t5_saved, vit_top_grad, t5_top_grad):
    sections = lax.axis_size("section")
    parts = lax.axis_size("dp")
    weights = [feature_groups(w[0], parts) for w in (t5_weight, vit_weight)]
    saveds = [feature_groups(s[0], parts) for s in (t5_saved, vit_saved)]
    tops = [feature_groups(t, parts) for t in (t5_top_grad, vit_top_grad)]
    micros, tokens = t5_top_grad.shape[:2]
    scale = 1.0 / (micros * tokens)
    results = branch_call(sections, weights, saveds, tops)
    grads, sums = [], []
    for b in range(2):
        out, columns, local = results[3 * b : 3 * b + 3]
        grads.append(jnp.moveaxis(out, 0, 2).reshape(micros, tokens, -1)[None])
        sums.append(weight_rows(columns, local, scale)[None])
    return (grads[1], grads[0], sums[1], sums[0])


def solution(mesh):
    placed = (
        P("section", "dp", None),
        P("section", "dp", None),
        P("section", None, "dp", None),
        P("section", None, "dp", None),
        P(None, "dp", None),
        P(None, "dp", None),
    )
    return jax.shard_map(
        shards,
        mesh=mesh,
        in_specs=placed,
        out_specs=(
            P("section", None, "dp", None),
            P("section", None, "dp", None),
            P("section", "dp", None),
            P("section", "dp", None),
        ),
        check_vma=False,
    )
```

```python
import functools

import jax
import jax.numpy as jnp
from jax import lax
from jax.experimental import pallas as pl
from jax.experimental.pallas import tpu as pltpu
from jax.sharding import PartitionSpec as P

root_half = 0.7071067811865476
inv_root_tau = 0.3989422804014327
MESH = pl.DeviceIdType.MESH


def gelu_slope(preact):
    cumulative = 0.5 * (1.0 + lax.erf(preact * root_half))
    density = jnp.exp(-0.5 * preact * preact) * inv_root_tau
    return cumulative + preact * density


class Branch:
    def __init__(self, ins, outs, scratch):
        self.weight, self.saved, self.top = ins
        self.out, self.columns, self.local = outs
        (
            self.above,
            self.below,
            self.mine,
            self.pair_out,
            self.pair_in,
            self.chip_in,
            self.slope,
            self.saved_sem,
            self.top_sem,
            self.pair_sem,
            self.chip_sem,
            self.near_sem,
            self.far_sem,
            self.hop_sem,
            self.out_sem,
        ) = scratch


BRANCH_SCRATCH = 15


def kernel(sections, parts, micros, *refs):
    ins, outs, scratch = refs[:6], refs[6:12], refs[12:]
    branches = [
        Branch(ins[3 * b : 3 * b + 3], outs[3 * b : 3 * b + 3],
               scratch[BRANCH_SCRATCH * b : BRANCH_SCRATCH * (b + 1)])
        for b in range(2)
    ]
    section = lax.axis_index("section")
    me = lax.axis_index("dp")
    chips = parts // 2
    chip, core = me // 2, me % 2
    partner = chip * 2 + 1 - core
    is_last = section == sections - 1
    is_first = section == 0

    def ahead(k):
        return lax.rem(chip + k, chips) * 2 + core

    def behind(k):
        return lax.rem(chip + chips - k, chips) * 2 + core

    def other(group):
        return group + 1 - 2 * core

    def copy(src, dst, sems, index, where, part):
        return pltpu.make_async_remote_copy(
            src_ref=src, dst_ref=dst, send_sem=sems.at[(0, *index)], recv_sem=sems.at[(1, *index)],
            device_id=(where, part), device_id_type=MESH,
        )

    barrier = pltpu.get_barrier_semaphore()
    for k in range(1, parts):
        pl.semaphore_signal(barrier, inc=1, device_id=(section, lax.rem(me + k, parts)), device_id_type=MESH)

    @pl.when(section > 0)
    def _():
        pl.semaphore_signal(barrier, inc=1, device_id=(section - 1, me), device_id_type=MESH)

    @pl.when(section < sections - 1)
    def _():
        pl.semaphore_signal(barrier, inc=1, device_id=(section + 1, me), device_id_type=MESH)

    neighbours = lax.min(section, 1) + lax.min(sections - 1 - section, 1)
    pl.semaphore_wait(barrier, parts - 1 + neighbours)

    def saved_copy(br, m, k):
        to = lax.rem(me + k, parts)
        return copy(br.saved.at[to, m], br.columns.at[m, me], br.saved_sem, (m, k - 1), section, to)

    def top_copy(br, m, k):
        to = lax.rem(me + k, parts)
        return copy(br.top.at[to, m], br.above.at[m, me], br.top_sem, (m, k - 1), section, to)

    def pair_copy(br, m):
        return copy(br.pair_out.at[m], br.pair_in.at[m], br.pair_sem, (m,), section, partner)

    def chip_copy(br, m, k):
        return copy(br.mine.at[m, k], br.chip_in.at[m, k - 1], br.chip_sem, (m, k - 1), section, ahead(k))

    def near_copy(br, m, k):
        group = behind(k)
        return copy(br.local.at[m, group], br.local.at[m, group], br.near_sem, (m, k), section, partner)

    def far_copy(br, m, k):
        return copy(br.local.at[m, me], br.local.at[m, me], br.far_sem, (m, k - 1), section, ahead(k))

    def hop_copy(br, m):
        return copy(br.below.at[m], br.above.at[m], br.hop_sem, (m,), lax.max(section - 1, 0), me)

    def out_copy(br, m, k):
        to = lax.rem(me + k, parts)
        return copy(br.below.at[m, to], br.out.at[me, m], br.out_sem, (m, k - 1), section, to)

    def rows(block):
        return block.reshape(-1, block.shape[-1])

    def send_saved(m):
        for br in branches:
            for k in range(1, parts):
                saved_copy(br, m, k).start()

    def send_top(m):
        for br in branches:
            for k in range(1, parts):
                top_copy(br, m, k).start()

    def partial(half):
        size = micros // 2
        first = half * size

        @pl.loop(first, first + size)
        def _(m):
            for br in branches:
                br.columns[m, me] = br.saved[me, m]
                for k in range(1, parts):
                    saved_copy(br, m, k).wait_recv()

        span = pl.ds(first, size)
        for br in branches:
            tokens = rows(br.columns[span])

            def product(group):
                block = jnp.dot(tokens, br.weight[group], preferred_element_type=jnp.float32)
                return block.astype(jnp.bfloat16).reshape(size, -1, block.shape[-1])

            for k in range(chips):
                br.pair_out[span, k] = product(other(ahead(k)))

            @pl.loop(first, first + size)
            def _(m):
                pair_copy(br, m).start()

            for k in range(chips):
                br.mine[span, k] = product(ahead(k))

    def pair_sum(m):
        for br in branches:
            pair_copy(br, m).wait_recv()
            for k in range(1, chips):
                both = br.mine[m, k].astype(jnp.float32) + br.pair_in[m, k].astype(jnp.float32)
                br.mine[m, k] = both.astype(jnp.bfloat16)
                chip_copy(br, m, k).start()

    def find_slope(br, m):
        total = br.mine[m, 0].astype(jnp.float32) + br.pair_in[m, 0].astype(jnp.float32)
        for k in range(1, chips):
            chip_copy(br, m, k).wait_recv()
            total = total + br.chip_in[m, k - 1].astype(jnp.float32)
        br.slope[m] = gelu_slope(total)

    def spread(m):
        for br in branches:
            @pl.when(is_last)
            def _():
                find_slope(br, m)
                br.above[m, me] = br.top[me, m]
                for k in range(1, parts):
                    top_copy(br, m, k).wait_recv()

            @pl.when(jnp.logical_not(is_last))
            def _():
                hop_copy(br, m).wait_recv()

            br.local[m, me] = (rows(br.above[m]).astype(jnp.float32) * br.slope[m]).astype(jnp.bfloat16)
            for k in range(1, chips):
                far_copy(br, m, k).start()
            near_copy(br, m, 0).start()

    def descend(m):
        for br in branches:
            def through(group):
                return lax.dot_general(
                    br.local[m, group], br.weight[group], (((1,), (1,)), ((), ())),
                    preferred_element_type=jnp.float32,
                )

            for k in range(1, chips):
                far_copy(br, m, k).wait_recv()
                near_copy(br, m, k).start()
            total = rows(br.above[m]).astype(jnp.float32) + through(me)
            near_copy(br, m, 0).wait_recv()
            total = total + through(partner)
            for k in range(1, chips):
                total = total + through(behind(k))
            for k in range(1, chips):
                near_copy(br, m, k).wait_recv()
                total = total + through(other(behind(k)))
            br.below[m] = total.astype(jnp.bfloat16).reshape(br.below.shape[1:])

            @pl.when(jnp.logical_not(is_first))
            def _():
                hop_copy(br, m).start()

    def hand_out(m):
        for br in branches:
            br.out[me, m] = br.below[m, me]
            for k in range(1, parts):
                out_copy(br, m, k).start()

    ready = min(2, micros)
    pl.loop(0, micros)(send_saved)

    @pl.when(is_last)
    def _():
        pl.loop(0, ready)(send_top)

    pl.loop(0, 2)(partial)

    @pl.when(is_last)
    def _():
        pl.loop(0, ready)(pair_sum)

    @pl.when(jnp.logical_not(is_last))
    def _():
        pl.loop(0, micros)(pair_sum)

        @pl.loop(0, micros)
        def _(m):
            for br in branches:
                find_slope(br, m)

    @pl.loop(0, micros + 1)
    def _(step):
        @pl.when(step < micros)
        def _():
            spread(step)

        @pl.when(jnp.logical_and(is_last, step < micros - ready))
        def _():
            pair_sum(step + ready)
            send_top(step + ready)

        @pl.when(step > 0)
        def _():
            descend(step - 1)

        @pl.when(jnp.logical_and(section < 2, step > 0))
        def _():
            hand_out(step - 1)

    @pl.when(section >= 2)
    def _():
        pl.loop(0, micros)(hand_out)

    @pl.loop(0, micros)
    def _(m):
        for br in branches:
            for k in range(1, parts):
                saved_copy(br, m, k).wait_send()
                out_copy(br, m, k).wait_send()
                out_copy(br, m, k).wait_recv()

            @pl.when(is_last)
            def _():
                for k in range(1, parts):
                    top_copy(br, m, k).wait_send()

            @pl.when(jnp.logical_not(is_first))
            def _():
                hop_copy(br, m).wait_send()

            pair_copy(br, m).wait_send()
            near_copy(br, m, 0).wait_send()
            for k in range(1, chips):
                chip_copy(br, m, k).wait_send()
                far_copy(br, m, k).wait_send()
                near_copy(br, m, k).wait_send()


def branch_call(sections, weights, saveds, tops):
    operands, outs, scratch = [], [], []
    for weight, saved, top in zip(weights, saveds, tops):
        parts, rows, _ = weight.shape
        micros, tokens = saved.shape[1:3]
        chips = parts // 2
        everyone = parts * tokens
        operands += [weight, saved, top]
        outs += [
            jax.ShapeDtypeStruct((parts, micros, tokens, rows), jnp.bfloat16),
            jax.ShapeDtypeStruct((micros, parts, tokens, rows), jnp.bfloat16),
            jax.ShapeDtypeStruct((micros, parts, everyone, rows), jnp.bfloat16),
        ]
        dma = pltpu.SemaphoreType.DMA
        scratch += [
            pltpu.VMEM((micros, parts, tokens, rows), jnp.bfloat16),
            pltpu.VMEM((micros, parts, tokens, rows), jnp.bfloat16),
            pltpu.VMEM((micros, chips, everyone, rows), jnp.bfloat16),
            pltpu.VMEM((micros, chips, everyone, rows), jnp.bfloat16),
            pltpu.VMEM((micros, chips, everyone, rows), jnp.bfloat16),
            pltpu.VMEM((micros, max(chips - 1, 1), everyone, rows), jnp.bfloat16),
            pltpu.VMEM((micros, everyone, rows), jnp.float32),
            dma((2, micros, parts - 1)),
            dma((2, micros, parts - 1)),
            dma((2, micros)),
            dma((2, micros, max(chips - 1, 1))),
            dma((2, micros, chips)),
            dma((2, micros, max(chips - 1, 1))),
            dma((2, micros)),
            dma((2, micros, parts - 1)),
        ]
    vmem = pl.BlockSpec(memory_space=pltpu.VMEM)
    return pl.pallas_call(
        functools.partial(kernel, sections, parts, micros),
        out_shape=outs,
        in_specs=[vmem] * len(operands),
        out_specs=[vmem] * len(outs),
        scratch_shapes=scratch,
        compiler_params=pltpu.CompilerParams(
            collective_id=0, has_side_effects=True, vmem_limit_bytes=60 * 1024 * 1024
        ),
    )(*operands)


def feature_groups(block, parts):
    return jnp.moveaxis(block.reshape(*block.shape[:-1], parts, -1), -2, 0)


def weight_rows(columns, locals_all, scale):
    micros, parts, tokens, rows = columns.shape
    columns = columns.astype(jnp.bfloat16)
    by_group = locals_all.reshape(micros, parts, parts, tokens, rows)
    total = None
    for group in range(parts):
        left = columns[:, group].reshape(-1, rows)
        right = by_group[:, :, group].transpose(0, 2, 1, 3).reshape(micros * tokens, -1)
        term = lax.dot_general(
            left, right, (((0,), (0,)), ((), ())), preferred_element_type=jnp.float32
        )
        term = (term * scale).astype(jnp.bfloat16).astype(jnp.float32)
        total = term if total is None else total + term
    return total


def shards(vit_weight, t5_weight, vit_saved, t5_saved, vit_top_grad, t5_top_grad):
    sections = lax.axis_size("section")
    parts = lax.axis_size("dp")
    weights = [feature_groups(w[0], parts) for w in (t5_weight, vit_weight)]
    micros, tokens = t5_top_grad.shape[:2]
    scale = 1.0 / (micros * tokens)
    cut = 2 if tokens % 32 == 0 else 1

    def chunks(block):
        return feature_groups(block.reshape(micros * cut, tokens // cut, -1), parts)

    saveds = [chunks(s) for s in (t5_saved, vit_saved)]
    tops = [chunks(t) for t in (t5_top_grad, vit_top_grad)]
    results = branch_call(sections, weights, saveds, tops)
    grads, sums = [], []
    for b in range(2):
        out, columns, local = results[3 * b : 3 * b + 3]
        grads.append(jnp.moveaxis(out, 0, 2).reshape(micros, tokens, -1)[None])
        sums.append(weight_rows(columns, local, scale)[None])
    return (grads[1], grads[0], sums[1], sums[0])


def solution(mesh):
    placed = (
        P("section", "dp", None),
        P("section", "dp", None),
        P("section", None, "dp", None),
        P("section", None, "dp", None),
        P(None, "dp", None),
        P(None, "dp", None),
    )
    return jax.shard_map(
        shards,
        mesh=mesh,
        in_specs=placed,
        out_specs=(
            P("section", None, "dp", None),
            P("section", None, "dp", None),
            P("section", "dp", None),
            P("section", "dp", None),
        ),
        check_vma=False,
    )
```

```python
import functools

import jax
import jax.numpy as jnp
from jax import lax
from jax.experimental import pallas as pl
from jax.experimental.pallas import tpu as pltpu
from jax.sharding import PartitionSpec as P

root_half = 0.7071067811865476
inv_root_tau = 0.3989422804014327
MESH = pl.DeviceIdType.MESH


def gelu_slope(preact):
    cumulative = 0.5 * (1.0 + lax.erf(preact * root_half))
    density = jnp.exp(-0.5 * preact * preact) * inv_root_tau
    return cumulative + preact * density


class Branch:
    def __init__(self, ins, outs, scratch):
        self.weight_in, self.saved_in, self.top_in = ins
        self.out, self.columns, self.local = outs
        (
            self.weight,
            self.saved,
            self.top,
            self.above,
            self.below,
            self.mine,
            self.pair_out,
            self.pair_in,
            self.chip_in,
            self.slope,
            self.saved_sem,
            self.top_sem,
            self.pair_sem,
            self.chip_sem,
            self.near_sem,
            self.far_sem,
            self.hop_sem,
            self.out_sem,
        ) = scratch


BRANCH_SCRATCH = 18


def kernel(sections, parts, micros, *refs):
    ins, outs, scratch = refs[:6], refs[6:12], refs[12:]
    branches = [
        Branch(ins[3 * b : 3 * b + 3], outs[3 * b : 3 * b + 3],
               scratch[BRANCH_SCRATCH * b : BRANCH_SCRATCH * (b + 1)])
        for b in range(2)
    ]
    section = lax.axis_index("section")
    me = lax.axis_index("dp")
    chips = parts // 2
    chip, core = me // 2, me % 2
    partner = chip * 2 + 1 - core
    is_last = section == sections - 1
    is_first = section == 0

    def ahead(k):
        return lax.rem(chip + k, chips) * 2 + core

    def behind(k):
        return lax.rem(chip + chips - k, chips) * 2 + core

    def other(group):
        return group + 1 - 2 * core

    def copy(src, dst, sems, index, where, part):
        return pltpu.make_async_remote_copy(
            src_ref=src, dst_ref=dst, send_sem=sems.at[(0, *index)], recv_sem=sems.at[(1, *index)],
            device_id=(where, part), device_id_type=MESH,
        )

    def regroup(source, groups):
        size = groups.shape[-1]
        for group in range(parts):
            groups[group] = source[..., group * size : (group + 1) * size]

    barrier = pltpu.get_barrier_semaphore()
    for k in range(1, parts):
        pl.semaphore_signal(barrier, inc=1, device_id=(section, lax.rem(me + k, parts)), device_id_type=MESH)

    @pl.when(section > 0)
    def _():
        pl.semaphore_signal(barrier, inc=1, device_id=(section - 1, me), device_id_type=MESH)

    @pl.when(section < sections - 1)
    def _():
        pl.semaphore_signal(barrier, inc=1, device_id=(section + 1, me), device_id_type=MESH)

    for br in branches:
        regroup(br.saved_in, br.saved)
    neighbours = lax.min(section, 1) + lax.min(sections - 1 - section, 1)
    pl.semaphore_wait(barrier, parts - 1 + neighbours)

    def saved_copy(br, m, k):
        to = lax.rem(me + k, parts)
        return copy(br.saved.at[to, m], br.columns.at[m, me], br.saved_sem, (m, k - 1), section, to)

    def top_copy(br, m, k):
        to = lax.rem(me + k, parts)
        return copy(br.top.at[to, m], br.above.at[m, me], br.top_sem, (m, k - 1), section, to)

    def pair_copy(br, m):
        return copy(br.pair_out.at[m], br.pair_in.at[m], br.pair_sem, (m,), section, partner)

    def chip_copy(br, m, k):
        return copy(br.mine.at[m, k], br.chip_in.at[m, k - 1], br.chip_sem, (m, k - 1), section, ahead(k))

    def near_copy(br, m, k):
        group = behind(k)
        return copy(br.local.at[m, group], br.local.at[m, group], br.near_sem, (m, k), section, partner)

    def far_copy(br, m, k):
        return copy(br.local.at[m, me], br.local.at[m, me], br.far_sem, (m, k - 1), section, ahead(k))

    def hop_copy(br, m):
        return copy(br.below.at[m], br.above.at[m], br.hop_sem, (m,), lax.max(section - 1, 0), me)

    def out_copy(br, m, k):
        to = lax.rem(me + k, parts)
        return copy(br.below.at[m, to], br.out.at[me, m], br.out_sem, (m, k - 1), section, to)

    def rows(block):
        return block.reshape(-1, block.shape[-1])

    def send_saved(m):
        for br in branches:
            for k in range(1, parts):
                saved_copy(br, m, k).start()

    def send_top(m):
        for br in branches:
            for k in range(1, parts):
                top_copy(br, m, k).start()

    def partial(half):
        size = micros // 2
        first = half * size

        @pl.loop(first, first + size)
        def _(m):
            for br in branches:
                br.columns[m, me] = br.saved[me, m]
                for k in range(1, parts):
                    saved_copy(br, m, k).wait_recv()

        span = pl.ds(first, size)
        for br in branches:
            tokens = rows(br.columns[span])

            def product(group):
                block = jnp.dot(tokens, br.weight[group], preferred_element_type=jnp.float32)
                return block.astype(jnp.bfloat16).reshape(size, -1, block.shape[-1])

            for k in range(chips):
                br.pair_out[span, k] = product(other(ahead(k)))

            @pl.loop(first, first + size)
            def _(m):
                pair_copy(br, m).start()

            for k in range(chips):
                br.mine[span, k] = product(ahead(k))

    def pair_sum(m):
        for br in branches:
            pair_copy(br, m).wait_recv()
            for k in range(1, chips):
                both = br.mine[m, k].astype(jnp.float32) + br.pair_in[m, k].astype(jnp.float32)
                br.mine[m, k] = both.astype(jnp.bfloat16)
                chip_copy(br, m, k).start()

    def find_slope(br, m):
        total = br.mine[m, 0].astype(jnp.float32) + br.pair_in[m, 0].astype(jnp.float32)
        for k in range(1, chips):
            chip_copy(br, m, k).wait_recv()
            total = total + br.chip_in[m, k - 1].astype(jnp.float32)
        br.slope[m] = gelu_slope(total)

    def spread(m):
        for br in branches:
            @pl.when(is_last)
            def _():
                find_slope(br, m)
                br.above[m, me] = br.top[me, m]
                for k in range(1, parts):
                    top_copy(br, m, k).wait_recv()

            @pl.when(jnp.logical_not(is_last))
            def _():
                hop_copy(br, m).wait_recv()

            br.local[m, me] = (rows(br.above[m]).astype(jnp.float32) * br.slope[m]).astype(jnp.bfloat16)
            for k in range(1, chips):
                far_copy(br, m, k).start()
            near_copy(br, m, 0).start()

    def descend(m):
        for br in branches:
            def through(group):
                return lax.dot_general(
                    br.local[m, group], br.weight[group], (((1,), (1,)), ((), ())),
                    preferred_element_type=jnp.float32,
                )

            for k in range(1, chips):
                far_copy(br, m, k).wait_recv()
                near_copy(br, m, k).start()
            total = rows(br.above[m]).astype(jnp.float32) + through(me)
            near_copy(br, m, 0).wait_recv()
            total = total + through(partner)
            for k in range(1, chips):
                total = total + through(behind(k))
            for k in range(1, chips):
                near_copy(br, m, k).wait_recv()
                total = total + through(other(behind(k)))
            br.below[m] = total.astype(jnp.bfloat16).reshape(br.below.shape[1:])

            @pl.when(jnp.logical_not(is_first))
            def _():
                hop_copy(br, m).start()

    def hand_out(m):
        for br in branches:
            br.out[me, m] = br.below[m, me]
            for k in range(1, parts):
                out_copy(br, m, k).start()

    ready = min(2, micros)
    pl.loop(0, micros)(send_saved)

    @pl.when(is_last)
    def _():
        for br in branches:
            regroup(br.top_in, br.top)
        pl.loop(0, ready)(send_top)

    for br in branches:
        regroup(br.weight_in, br.weight)

    pl.loop(0, 2)(partial)

    @pl.when(is_last)
    def _():
        pl.loop(0, ready)(pair_sum)

    @pl.when(jnp.logical_not(is_last))
    def _():
        pl.loop(0, micros)(pair_sum)

        @pl.loop(0, micros)
        def _(m):
            for br in branches:
                find_slope(br, m)

    @pl.loop(0, micros + 1)
    def _(step):
        @pl.when(step < micros)
        def _():
            spread(step)

        @pl.when(jnp.logical_and(is_last, step < micros - ready))
        def _():
            pair_sum(step + ready)
            send_top(step + ready)

        @pl.when(step > 0)
        def _():
            descend(step - 1)

        @pl.when(jnp.logical_and(section < 2, step > 0))
        def _():
            hand_out(step - 1)

    @pl.when(section >= 2)
    def _():
        pl.loop(0, micros)(hand_out)

    @pl.loop(0, micros)
    def _(m):
        for br in branches:
            for k in range(1, parts):
                saved_copy(br, m, k).wait_send()
                out_copy(br, m, k).wait_send()
                out_copy(br, m, k).wait_recv()

            @pl.when(is_last)
            def _():
                for k in range(1, parts):
                    top_copy(br, m, k).wait_send()

            @pl.when(jnp.logical_not(is_first))
            def _():
                hop_copy(br, m).wait_send()

            pair_copy(br, m).wait_send()
            near_copy(br, m, 0).wait_send()
            for k in range(1, chips):
                chip_copy(br, m, k).wait_send()
                far_copy(br, m, k).wait_send()
                near_copy(br, m, k).wait_send()


def branch_call(sections, weights, saveds, tops):
    operands, outs, scratch = [], [], []
    for weight, saved, top in zip(weights, saveds, tops):
        rows, width = weight.shape
        micros, tokens = saved.shape[:2]
        parts = width // rows
        chips = parts // 2
        everyone = parts * tokens
        operands += [weight, saved, top]
        outs += [
            jax.ShapeDtypeStruct((parts, micros, tokens, rows), jnp.bfloat16),
            jax.ShapeDtypeStruct((micros, parts, tokens, rows), jnp.bfloat16),
            jax.ShapeDtypeStruct((micros, parts, everyone, rows), jnp.bfloat16),
        ]
        dma = pltpu.SemaphoreType.DMA
        scratch += [
            pltpu.VMEM((parts, rows, rows), jnp.bfloat16),
            pltpu.VMEM((parts, micros, tokens, rows), jnp.bfloat16),
            pltpu.VMEM((parts, micros, tokens, rows), jnp.bfloat16),
            pltpu.VMEM((micros, parts, tokens, rows), jnp.bfloat16),
            pltpu.VMEM((micros, parts, tokens, rows), jnp.bfloat16),
            pltpu.VMEM((micros, chips, everyone, rows), jnp.bfloat16),
            pltpu.VMEM((micros, chips, everyone, rows), jnp.bfloat16),
            pltpu.VMEM((micros, chips, everyone, rows), jnp.bfloat16),
            pltpu.VMEM((micros, max(chips - 1, 1), everyone, rows), jnp.bfloat16),
            pltpu.VMEM((micros, everyone, rows), jnp.float32),
            dma((2, micros, parts - 1)),
            dma((2, micros, parts - 1)),
            dma((2, micros)),
            dma((2, micros, max(chips - 1, 1))),
            dma((2, micros, chips)),
            dma((2, micros, max(chips - 1, 1))),
            dma((2, micros)),
            dma((2, micros, parts - 1)),
        ]
    vmem = pl.BlockSpec(memory_space=pltpu.VMEM)
    return pl.pallas_call(
        functools.partial(kernel, sections, parts, micros),
        out_shape=outs,
        in_specs=[vmem] * len(operands),
        out_specs=[vmem] * len(outs),
        scratch_shapes=scratch,
        compiler_params=pltpu.CompilerParams(
            collective_id=0, has_side_effects=True, vmem_limit_bytes=60 * 1024 * 1024
        ),
    )(*operands)


def finish_kernel(scale, *refs):
    outs, buffers, sems = refs[6:10], refs[10:14], refs[14]
    pending = []

    def flush(src, dst):
        copy = pltpu.make_async_copy(src, dst, sems.at[len(pending)])
        copy.start()
        pending.append(copy)

    for b in (1, 0):
        grads_in, columns, local = refs[3 * b : 3 * b + 3]
        grads, sums = outs[2 * b : 2 * b + 2]
        grad_buffer, sum_buffer = buffers[2 * b : 2 * b + 2]
        micros, parts, tokens, rows = columns.shape
        for part in range(parts):
            grad_buffer[:, :, part * rows : (part + 1) * rows] = grads_in[part]
        flush(grad_buffer, grads)
        lefts = [columns[:, group].reshape(micros * tokens, rows) for group in range(parts)]
        for part in range(parts):
            span = pl.ds(part * rows, rows)
            total = None
            for group in range(parts):
                right = local[:, part, group * tokens : (group + 1) * tokens]
                term = lax.dot_general(
                    lefts[group], right.reshape(micros * tokens, rows), (((0,), (0,)), ((), ())),
                    preferred_element_type=jnp.float32,
                )
                term = (term * scale).astype(jnp.bfloat16).astype(jnp.float32)
                total = term if total is None else total + term
            sum_buffer[:, part * rows : (part + 1) * rows] = total
            if rows % 128 == 0:
                flush(sum_buffer.at[:, span], sums.at[:, span])
        if rows % 128:
            flush(sum_buffer, sums)
    for copy in pending:
        copy.wait()


def finish(results, scale):
    outs, buffers = [], []
    for b in range(2):
        parts, micros, tokens, rows = results[3 * b].shape
        shapes = [((micros, tokens, parts * rows), jnp.bfloat16), ((rows, parts * rows), jnp.float32)]
        outs += [jax.ShapeDtypeStruct(*shape) for shape in shapes]
        buffers += [pltpu.VMEM(*shape) for shape in shapes]
    return pl.pallas_call(
        functools.partial(finish_kernel, scale),
        out_shape=outs,
        in_specs=[pl.BlockSpec(memory_space=pltpu.VMEM)] * 6,
        out_specs=[pl.BlockSpec(memory_space=pl.ANY)] * 4,
        scratch_shapes=buffers + [pltpu.SemaphoreType.DMA((2 * parts + 4,))],
        compiler_params=pltpu.CompilerParams(vmem_limit_bytes=40 * 1024 * 1024),
    )(*results)


def shards(vit_weight, t5_weight, vit_saved, t5_saved, vit_top_grad, t5_top_grad):
    sections = lax.axis_size("section")
    micros, tokens = t5_top_grad.shape[:2]
    scale = 1.0 / (micros * tokens)
    cut = 2 if tokens % 32 == 0 else 1

    def chunks(block):
        return block.reshape(micros * cut, tokens // cut, -1)

    results = branch_call(
        sections,
        [t5_weight[0], vit_weight[0]],
        [chunks(t5_saved[0]), chunks(vit_saved[0])],
        [chunks(t5_top_grad), chunks(vit_top_grad)],
    )
    t5_grads, t5_sum, vit_grads, vit_sum = finish(results, scale)
    return (
        vit_grads.reshape(vit_saved.shape),
        t5_grads.reshape(t5_saved.shape),
        vit_sum[None],
        t5_sum[None],
    )


def solution(mesh):
    placed = (
        P("section", "dp", None),
        P("section", "dp", None),
        P("section", None, "dp", None),
        P("section", None, "dp", None),
        P(None, "dp", None),
        P(None, "dp", None),
    )
    return jax.shard_map(
        shards,
        mesh=mesh,
        in_specs=placed,
        out_specs=(
            P("section", None, "dp", None),
            P("section", None, "dp", None),
            P("section", "dp", None),
            P("section", "dp", None),
        ),
        check_vma=False,
    )
```

```python
import functools

import jax
import jax.numpy as jnp
from jax import lax
from jax.experimental import pallas as pl
from jax.experimental.pallas import tpu as pltpu
from jax.sharding import PartitionSpec as P

root_half = 0.7071067811865476
inv_root_tau = 0.3989422804014327
MESH = pl.DeviceIdType.MESH


def gelu_slope(preact):
    cumulative = 0.5 * (1.0 + lax.erf(preact * root_half))
    density = jnp.exp(-0.5 * preact * preact) * inv_root_tau
    return cumulative + preact * density


class Branch:
    def __init__(self, ins, outs, scratch):
        self.weight_in, self.saved_in, self.top_in = ins
        self.out, self.columns, self.local = outs
        (
            self.weight,
            self.saved,
            self.top,
            self.above,
            self.lifted,
            self.lift_sem,
            self.below,
            self.mine,
            self.pair_out,
            self.pair_in,
            self.chip_in,
            self.slope,
            self.saved_sem,
            self.top_sem,
            self.pair_sem,
            self.chip_sem,
            self.near_sem,
            self.far_sem,
            self.hop_sem,
            self.out_sem,
        ) = scratch


BRANCH_SCRATCH = 20


def kernel(sections, parts, micros, *refs):
    ins, outs, scratch = refs[:6], refs[6:12], refs[12:]
    branches = [
        Branch(ins[3 * b : 3 * b + 3], outs[3 * b : 3 * b + 3],
               scratch[BRANCH_SCRATCH * b : BRANCH_SCRATCH * (b + 1)])
        for b in range(2)
    ]
    section = lax.axis_index("section")
    me = lax.axis_index("dp")
    chips = parts // 2
    chip, core = me // 2, me % 2
    partner = chip * 2 + 1 - core
    is_last = section == sections - 1
    is_first = section == 0

    def ahead(k):
        return lax.rem(chip + k, chips) * 2 + core

    def behind(k):
        return lax.rem(chip + chips - k, chips) * 2 + core

    def other(group):
        return group + 1 - 2 * core

    def copy(src, dst, sems, index, where, part):
        return pltpu.make_async_remote_copy(
            src_ref=src, dst_ref=dst, send_sem=sems.at[(0, *index)], recv_sem=sems.at[(1, *index)],
            device_id=(where, part), device_id_type=MESH,
        )

    def regroup(source, groups):
        size = groups.shape[-1]
        for group in range(parts):
            groups[group] = source[..., group * size : (group + 1) * size]

    barrier = pltpu.get_barrier_semaphore()
    for k in range(1, parts):
        pl.semaphore_signal(barrier, inc=1, device_id=(section, lax.rem(me + k, parts)), device_id_type=MESH)

    def greet(other_section):
        pl.semaphore_signal(barrier, inc=1, device_id=(other_section, me), device_id_type=MESH)

    @pl.when(is_last)
    def _():
        pl.loop(0, sections - 1)(greet)

    @pl.when(jnp.logical_not(is_last))
    def _():
        greet(sections - 1)

        @pl.when(section > 0)
        def _():
            greet(section - 1)

        @pl.when(section < sections - 2)
        def _():
            greet(section + 1)

    for br in branches:
        regroup(br.saved_in, br.saved)
    below_last = lax.min(sections - 1 - section, 1)
    column = below_last * (1 + lax.min(section, 1) + lax.min(lax.max(sections - 2 - section, 0), 1))
    pl.semaphore_wait(barrier, parts - 1 + column + (1 - below_last) * (sections - 1))

    def saved_copy(br, m, k):
        to = lax.rem(me + k, parts)
        return copy(br.saved.at[to, m], br.columns.at[m, me], br.saved_sem, (m, k - 1), section, to)

    def top_copy(br, m, k):
        to = lax.rem(me + k, parts)
        return copy(br.top.at[to, m], br.lifted.at[m, me], br.top_sem, (m, k - 1), section, to)

    def lift_copy(br, m):
        return copy(br.lifted.at[m], br.above.at[m], br.lift_sem, (m,), sections - 1, me)

    def helper(m):
        return sections - 1 - lax.rem(m, sections)

    def pair_copy(br, m):
        return copy(br.pair_out.at[m], br.pair_in.at[m], br.pair_sem, (m,), section, partner)

    def chip_copy(br, m, k):
        return copy(br.mine.at[m, k], br.chip_in.at[m, k - 1], br.chip_sem, (m, k - 1), section, ahead(k))

    def near_copy(br, m, k):
        group = behind(k)
        return copy(br.local.at[m, group], br.local.at[m, group], br.near_sem, (m, k), section, partner)

    def far_copy(br, m, k):
        return copy(br.local.at[m, me], br.local.at[m, me], br.far_sem, (m, k - 1), section, ahead(k))

    def hop_copy(br, m):
        return copy(br.below.at[m], br.above.at[m], br.hop_sem, (m,), lax.max(section - 1, 0), me)

    def out_copy(br, m, k):
        to = lax.rem(me + k, parts)
        return copy(br.below.at[m, to], br.out.at[me, m], br.out_sem, (m, k - 1), section, to)

    def rows(block):
        return block.reshape(-1, block.shape[-1])

    def send_saved(m):
        for br in branches:
            for k in range(1, parts):
                saved_copy(br, m, k).start()

    def send_top(m):
        for br in branches:
            for k in range(1, parts):
                top_copy(br, m, k).start()

    def partial(half):
        size = micros // 2
        first = half * size

        @pl.loop(first, first + size)
        def _(m):
            for br in branches:
                br.columns[m, me] = br.saved[me, m]
                for k in range(1, parts):
                    saved_copy(br, m, k).wait_recv()

        span = pl.ds(first, size)
        for br in branches:
            tokens = rows(br.columns[span])

            def product(group):
                block = jnp.dot(tokens, br.weight[group], preferred_element_type=jnp.float32)
                return block.astype(jnp.bfloat16).reshape(size, -1, block.shape[-1])

            for k in range(chips):
                br.pair_out[span, k] = product(other(ahead(k)))

            @pl.loop(first, first + size)
            def _(m):
                pair_copy(br, m).start()

            for k in range(chips):
                br.mine[span, k] = product(ahead(k))

    def pair_sum(m):
        for br in branches:
            pair_copy(br, m).wait_recv()
            for k in range(1, chips):
                both = br.mine[m, k].astype(jnp.float32) + br.pair_in[m, k].astype(jnp.float32)
                br.mine[m, k] = both.astype(jnp.bfloat16)
                chip_copy(br, m, k).start()

    def find_slope(br, m):
        total = br.mine[m, 0].astype(jnp.float32) + br.pair_in[m, 0].astype(jnp.float32)
        for k in range(1, chips):
            chip_copy(br, m, k).wait_recv()
            total = total + br.chip_in[m, k - 1].astype(jnp.float32)
        br.slope[m] = gelu_slope(total)

    def gather_top(br, m):
        br.lifted[m, me] = br.top[me, m]
        for k in range(1, parts):
            top_copy(br, m, k).wait_recv()

    def spread(m):
        for br in branches:
            @pl.when(is_last)
            def _():
                find_slope(br, m)

                @pl.when(helper(m) == section)
                def _():
                    gather_top(br, m)
                    br.above[m] = br.lifted[m]

                @pl.when(helper(m) != section)
                def _():
                    lift_copy(br, m).wait_recv()

            @pl.when(jnp.logical_not(is_last))
            def _():
                hop_copy(br, m).wait_recv()

            br.local[m, me] = (rows(br.above[m]).astype(jnp.float32) * br.slope[m]).astype(jnp.bfloat16)
            for k in range(1, chips):
                far_copy(br, m, k).start()
            near_copy(br, m, 0).start()

    def descend(m):
        for br in branches:
            def through(group):
                return lax.dot_general(
                    br.local[m, group], br.weight[group], (((1,), (1,)), ((), ())),
                    preferred_element_type=jnp.float32,
                )

            for k in range(1, chips):
                far_copy(br, m, k).wait_recv()
                near_copy(br, m, k).start()
            total = rows(br.above[m]).astype(jnp.float32) + through(me)
            near_copy(br, m, 0).wait_recv()
            total = total + through(partner)
            for k in range(1, chips):
                total = total + through(behind(k))
            for k in range(1, chips):
                near_copy(br, m, k).wait_recv()
                total = total + through(other(behind(k)))
            br.below[m] = total.astype(jnp.bfloat16).reshape(br.below.shape[1:])

            @pl.when(jnp.logical_not(is_first))
            def _():
                hop_copy(br, m).start()

    def hand_out(m):
        for br in branches:
            br.out[me, m] = br.below[m, me]
            for k in range(1, parts):
                out_copy(br, m, k).start()

    ready = min(2, micros)
    pl.loop(0, micros)(send_saved)

    for br in branches:
        regroup(br.top_in, br.top)

    @pl.loop(0, micros)
    def _(m):
        @pl.when(helper(m) == section)
        def _():
            send_top(m)

    for br in branches:
        regroup(br.weight_in, br.weight)

    pl.loop(0, 2)(partial)

    @pl.when(is_last)
    def _():
        pl.loop(0, ready)(pair_sum)

    @pl.when(jnp.logical_not(is_last))
    def _():
        @pl.loop(0, micros)
        def _(m):
            @pl.when(helper(m) == section)
            def _():
                for br in branches:
                    gather_top(br, m)
                    lift_copy(br, m).start()

        pl.loop(0, micros)(pair_sum)

        @pl.loop(0, micros)
        def _(m):
            for br in branches:
                find_slope(br, m)

    @pl.loop(0, micros + 1)
    def _(step):
        @pl.when(step < micros)
        def _():
            spread(step)

        @pl.when(jnp.logical_and(is_last, step < micros - ready))
        def _():
            pair_sum(step + ready)

        @pl.when(step > 0)
        def _():
            descend(step - 1)

        @pl.when(jnp.logical_and(section < 2, step > 0))
        def _():
            hand_out(step - 1)

    @pl.when(section >= 2)
    def _():
        pl.loop(0, micros)(hand_out)

    @pl.loop(0, micros)
    def _(m):
        for br in branches:
            for k in range(1, parts):
                saved_copy(br, m, k).wait_send()
                out_copy(br, m, k).wait_send()
                out_copy(br, m, k).wait_recv()

            @pl.when(helper(m) == section)
            def _():
                for k in range(1, parts):
                    top_copy(br, m, k).wait_send()

                @pl.when(jnp.logical_not(is_last))
                def _():
                    lift_copy(br, m).wait_send()

            @pl.when(jnp.logical_not(is_first))
            def _():
                hop_copy(br, m).wait_send()

            pair_copy(br, m).wait_send()
            near_copy(br, m, 0).wait_send()
            for k in range(1, chips):
                chip_copy(br, m, k).wait_send()
                far_copy(br, m, k).wait_send()
                near_copy(br, m, k).wait_send()


def branch_call(sections, weights, saveds, tops):
    operands, outs, scratch = [], [], []
    for weight, saved, top in zip(weights, saveds, tops):
        rows, width = weight.shape
        micros, tokens = saved.shape[:2]
        parts = width // rows
        chips = parts // 2
        everyone = parts * tokens
        operands += [weight, saved, top]
        outs += [
            jax.ShapeDtypeStruct((parts, micros, tokens, rows), jnp.bfloat16),
            jax.ShapeDtypeStruct((micros, parts, tokens, rows), jnp.bfloat16),
            jax.ShapeDtypeStruct((micros, parts, everyone, rows), jnp.bfloat16),
        ]
        dma = pltpu.SemaphoreType.DMA
        scratch += [
            pltpu.VMEM((parts, rows, rows), jnp.bfloat16),
            pltpu.VMEM((parts, micros, tokens, rows), jnp.bfloat16),
            pltpu.VMEM((parts, micros, tokens, rows), jnp.bfloat16),
            pltpu.VMEM((micros, parts, tokens, rows), jnp.bfloat16),
            pltpu.VMEM((micros, parts, tokens, rows), jnp.bfloat16),
            dma((2, micros)),
            pltpu.VMEM((micros, parts, tokens, rows), jnp.bfloat16),
            pltpu.VMEM((micros, chips, everyone, rows), jnp.bfloat16),
            pltpu.VMEM((micros, chips, everyone, rows), jnp.bfloat16),
            pltpu.VMEM((micros, chips, everyone, rows), jnp.bfloat16),
            pltpu.VMEM((micros, max(chips - 1, 1), everyone, rows), jnp.bfloat16),
            pltpu.VMEM((micros, everyone, rows), jnp.float32),
            dma((2, micros, parts - 1)),
            dma((2, micros, parts - 1)),
            dma((2, micros)),
            dma((2, micros, max(chips - 1, 1))),
            dma((2, micros, chips)),
            dma((2, micros, max(chips - 1, 1))),
            dma((2, micros)),
            dma((2, micros, parts - 1)),
        ]
    vmem = pl.BlockSpec(memory_space=pltpu.VMEM)
    return pl.pallas_call(
        functools.partial(kernel, sections, parts, micros),
        out_shape=outs,
        in_specs=[vmem] * len(operands),
        out_specs=[vmem] * len(outs),
        scratch_shapes=scratch,
        compiler_params=pltpu.CompilerParams(
            collective_id=0, has_side_effects=True, vmem_limit_bytes=60 * 1024 * 1024
        ),
    )(*operands)


def finish_kernel(scale, *refs):
    outs, buffers, sems = refs[6:10], refs[10:14], refs[14]
    staged, in_sems = refs[15:21], refs[21]
    loads = [pltpu.make_async_copy(refs[i], staged[i], in_sems.at[i]) for i in range(6)]
    for i in (3, 4, 5, 0, 1, 2):
        loads[i].start()
    pending = []

    def flush(src, dst):
        copy = pltpu.make_async_copy(src, dst, sems.at[len(pending)])
        copy.start()
        pending.append(copy)

    for b in (1, 0):
        grads_in, columns, local = staged[3 * b : 3 * b + 3]
        for load in loads[3 * b : 3 * b + 3]:
            load.wait()
        grads, sums = outs[2 * b : 2 * b + 2]
        grad_buffer, sum_buffer = buffers[2 * b : 2 * b + 2]
        micros, parts, tokens, rows = columns.shape
        for part in range(parts):
            grad_buffer[:, :, part * rows : (part + 1) * rows] = grads_in[part]
        flush(grad_buffer, grads)
        lefts = [columns[:, group].reshape(micros * tokens, rows) for group in range(parts)]
        for part in range(parts):
            span = pl.ds(part * rows, rows)
            total = None
            for group in range(parts):
                right = local[:, part, group * tokens : (group + 1) * tokens]
                term = lax.dot_general(
                    lefts[group], right.reshape(micros * tokens, rows), (((0,), (0,)), ((), ())),
                    preferred_element_type=jnp.float32,
                )
                term = (term * scale).astype(jnp.bfloat16).astype(jnp.float32)
                total = term if total is None else total + term
            sum_buffer[:, part * rows : (part + 1) * rows] = total
            if rows % 128 == 0:
                flush(sum_buffer.at[:, span], sums.at[:, span])
        if rows % 128:
            flush(sum_buffer, sums)
    for copy in pending:
        copy.wait()


def finish(results, scale):
    outs, buffers = [], []
    for b in range(2):
        parts, micros, tokens, rows = results[3 * b].shape
        shapes = [((micros, tokens, parts * rows), jnp.bfloat16), ((rows, parts * rows), jnp.float32)]
        outs += [jax.ShapeDtypeStruct(*shape) for shape in shapes]
        buffers += [pltpu.VMEM(*shape) for shape in shapes]
    return pl.pallas_call(
        functools.partial(finish_kernel, scale),
        out_shape=outs,
        in_specs=[pl.BlockSpec(memory_space=pl.ANY)] * 6,
        out_specs=[pl.BlockSpec(memory_space=pl.ANY)] * 4,
        scratch_shapes=buffers
        + [pltpu.SemaphoreType.DMA((2 * parts + 4,))]
        + [pltpu.VMEM(result.shape, result.dtype) for result in results]
        + [pltpu.SemaphoreType.DMA((6,))],
        compiler_params=pltpu.CompilerParams(vmem_limit_bytes=40 * 1024 * 1024),
    )(*results)


def shards(vit_weight, t5_weight, vit_saved, t5_saved, vit_top_grad, t5_top_grad):
    sections = lax.axis_size("section")
    micros, tokens = t5_top_grad.shape[:2]
    scale = 1.0 / (micros * tokens)
    cut = 2 if tokens % 32 == 0 else 1

    def chunks(block):
        return block.reshape(micros * cut, tokens // cut, -1)

    results = branch_call(
        sections,
        [t5_weight[0], vit_weight[0]],
        [chunks(t5_saved[0]), chunks(vit_saved[0])],
        [chunks(t5_top_grad), chunks(vit_top_grad)],
    )
    t5_grads, t5_sum, vit_grads, vit_sum = finish(results, scale)
    return (
        vit_grads.reshape(vit_saved.shape),
        t5_grads.reshape(t5_saved.shape),
        vit_sum[None],
        t5_sum[None],
    )


def solution(mesh):
    placed = (
        P("section", "dp", None),
        P("section", "dp", None),
        P("section", None, "dp", None),
        P("section", None, "dp", None),
        P(None, "dp", None),
        P(None, "dp", None),
    )
    return jax.shard_map(
        shards,
        mesh=mesh,
        in_specs=placed,
        out_specs=(
            P("section", None, "dp", None),
            P("section", None, "dp", None),
            P("section", "dp", None),
            P("section", "dp", None),
        ),
        check_vma=False,
    )
```

```python
import functools

import jax
import jax.numpy as jnp
from jax import lax
from jax.experimental import pallas as pl
from jax.experimental.pallas import tpu as pltpu
from jax.sharding import PartitionSpec as P

root_half = 0.7071067811865476
inv_root_tau = 0.3989422804014327
MESH = pl.DeviceIdType.MESH


def gelu_slope(preact):
    cumulative = 0.5 * (1.0 + lax.erf(preact * root_half))
    density = jnp.exp(-0.5 * preact * preact) * inv_root_tau
    return cumulative + preact * density


class Branch:
    def __init__(self, ins, outs, scratch):
        self.weight_in, self.saved_in, self.top_in = ins
        self.out, self.columns, self.local = outs
        (
            self.weight,
            self.saved,
            self.top,
            self.above,
            self.lifted,
            self.lift_sem,
            self.below,
            self.mine,
            self.pair_out,
            self.pair_in,
            self.chip_in,
            self.slope,
            self.saved_sem,
            self.top_sem,
            self.pair_sem,
            self.chip_sem,
            self.near_sem,
            self.far_sem,
            self.hop_sem,
            self.out_sem,
        ) = scratch


BRANCH_SCRATCH = 20


def kernel(sections, parts, micros, *refs):
    ins, outs, scratch = refs[:6], refs[6:12], refs[12:]
    branches = [
        Branch(ins[3 * b : 3 * b + 3], outs[3 * b : 3 * b + 3],
               scratch[BRANCH_SCRATCH * b : BRANCH_SCRATCH * (b + 1)])
        for b in range(2)
    ]
    section = lax.axis_index("section")
    me = lax.axis_index("dp")
    chips = parts // 2
    chip, core = me // 2, me % 2
    partner = chip * 2 + 1 - core
    is_last = section == sections - 1
    is_first = section == 0

    def ahead(k):
        return lax.rem(chip + k, chips) * 2 + core

    def behind(k):
        return lax.rem(chip + chips - k, chips) * 2 + core

    def other(group):
        return group + 1 - 2 * core

    def copy(src, dst, sems, index, where, part):
        return pltpu.make_async_remote_copy(
            src_ref=src, dst_ref=dst, send_sem=sems.at[(0, *index)], recv_sem=sems.at[(1, *index)],
            device_id=(where, part), device_id_type=MESH,
        )

    def regroup(source, groups):
        size = groups.shape[-1]
        for group in range(parts):
            groups[group] = source[..., group * size : (group + 1) * size]

    barrier = pltpu.get_barrier_semaphore()
    for k in range(1, parts):
        pl.semaphore_signal(barrier, inc=1, device_id=(section, lax.rem(me + k, parts)), device_id_type=MESH)

    def greet(other_section):
        pl.semaphore_signal(barrier, inc=1, device_id=(other_section, me), device_id_type=MESH)

    @pl.when(is_last)
    def _():
        pl.loop(0, sections - 1)(greet)

    @pl.when(jnp.logical_not(is_last))
    def _():
        greet(sections - 1)

        @pl.when(section > 0)
        def _():
            greet(section - 1)

        @pl.when(section < sections - 2)
        def _():
            greet(section + 1)

    for br in branches:
        regroup(br.saved_in, br.saved)
    below_last = lax.min(sections - 1 - section, 1)
    column = below_last * (1 + lax.min(section, 1) + lax.min(lax.max(sections - 2 - section, 0), 1))
    pl.semaphore_wait(barrier, parts - 1 + column + (1 - below_last) * (sections - 1))

    def saved_copy(br, m, k):
        to = lax.rem(me + k, parts)
        return copy(br.saved.at[to, m], br.columns.at[m, me], br.saved_sem, (m, k - 1), section, to)

    def top_copy(br, m, k):
        to = lax.rem(me + k, parts)
        return copy(br.top.at[to, m], br.lifted.at[m, me], br.top_sem, (m, k - 1), section, to)

    def lift_copy(br, m):
        return copy(br.lifted.at[m], br.above.at[m], br.lift_sem, (m,), sections - 1, me)

    def helper(m):
        return sections - 1 - lax.rem(m, sections)

    def pair_copy(br, m):
        return copy(br.pair_out.at[m], br.pair_in.at[m], br.pair_sem, (m,), section, partner)

    def chip_copy(br, m, k):
        return copy(br.mine.at[m, k], br.chip_in.at[m, k - 1], br.chip_sem, (m, k - 1), section, ahead(k))

    def near_copy(br, m, k):
        group = behind(k)
        return copy(br.local.at[m, group], br.local.at[m, group], br.near_sem, (m, k), section, partner)

    def far_copy(br, m, k):
        return copy(br.local.at[m, me], br.local.at[m, me], br.far_sem, (m, k - 1), section, ahead(k))

    def hop_copy(br, m):
        return copy(br.below.at[m], br.above.at[m], br.hop_sem, (m,), lax.max(section - 1, 0), me)

    def out_copy(br, m, k):
        to = lax.rem(me + k, parts)
        return copy(br.below.at[m, to], br.out.at[me, m], br.out_sem, (m, k - 1), section, to)

    def rows(block):
        return block.reshape(-1, block.shape[-1])

    def send_saved(m):
        for br in branches:
            for k in range(1, parts):
                saved_copy(br, m, k).start()

    def send_top(m):
        for br in branches:
            for k in range(1, parts):
                top_copy(br, m, k).start()

    def partial(half):
        size = micros // 2
        first = half * size

        @pl.loop(first, first + size)
        def _(m):
            for br in branches:
                br.columns[m, me] = br.saved[me, m]
                for k in range(1, parts):
                    saved_copy(br, m, k).wait_recv()

        span = pl.ds(first, size)
        for br in branches:
            tokens = rows(br.columns[span])

            def product(group):
                block = jnp.dot(tokens, br.weight[group], preferred_element_type=jnp.float32)
                return block.astype(jnp.bfloat16).reshape(size, -1, block.shape[-1])

            for k in range(chips):
                br.pair_out[span, k] = product(other(ahead(k)))

            @pl.loop(first, first + size)
            def _(m):
                pair_copy(br, m).start()

            for k in range(chips):
                br.mine[span, k] = product(ahead(k))

    def pair_sum(m):
        for br in branches:
            pair_copy(br, m).wait_recv()
            for k in range(1, chips):
                both = br.mine[m, k].astype(jnp.float32) + br.pair_in[m, k].astype(jnp.float32)
                br.mine[m, k] = both.astype(jnp.bfloat16)
                chip_copy(br, m, k).start()

    def find_slope(br, m):
        total = br.mine[m, 0].astype(jnp.float32) + br.pair_in[m, 0].astype(jnp.float32)
        for k in range(1, chips):
            chip_copy(br, m, k).wait_recv()
            total = total + br.chip_in[m, k - 1].astype(jnp.float32)
        br.slope[m] = gelu_slope(total)

    def gather_top(br, m):
        br.lifted[m, me] = br.top[me, m]
        for k in range(1, parts):
            top_copy(br, m, k).wait_recv()

    def spread(m):
        for br in branches:
            @pl.when(is_last)
            def _():
                find_slope(br, m)

                @pl.when(helper(m) == section)
                def _():
                    gather_top(br, m)
                    br.above[m] = br.lifted[m]

                @pl.when(helper(m) != section)
                def _():
                    lift_copy(br, m).wait_recv()

            @pl.when(jnp.logical_not(is_last))
            def _():
                hop_copy(br, m).wait_recv()

            br.local[m, me] = (rows(br.above[m]).astype(jnp.float32) * br.slope[m]).astype(jnp.bfloat16)
            for k in range(1, chips):
                far_copy(br, m, k).start()
            near_copy(br, m, 0).start()

    def descend(m):
        for br in branches:
            def through(group):
                return lax.dot_general(
                    br.local[m, group], br.weight[group], (((1,), (1,)), ((), ())),
                    preferred_element_type=jnp.float32,
                )

            for k in range(1, chips):
                far_copy(br, m, k).wait_recv()
                near_copy(br, m, k).start()
            total = rows(br.above[m]).astype(jnp.float32) + through(me)
            near_copy(br, m, 0).wait_recv()
            total = total + through(partner)
            for k in range(1, chips):
                total = total + through(behind(k))
            for k in range(1, chips):
                near_copy(br, m, k).wait_recv()
                total = total + through(other(behind(k)))
            br.below[m] = total.astype(jnp.bfloat16).reshape(br.below.shape[1:])

            @pl.when(jnp.logical_not(is_first))
            def _():
                hop_copy(br, m).start()

    def hand_out(m):
        for br in branches:
            br.out[me, m] = br.below[m, me]
            for k in range(1, parts):
                out_copy(br, m, k).start()

    ready = min(2, micros)
    pl.loop(0, micros)(send_saved)

    for br in branches:
        regroup(br.top_in, br.top)

    @pl.loop(0, micros)
    def _(m):
        @pl.when(helper(m) == section)
        def _():
            send_top(m)

    for br in branches:
        regroup(br.weight_in, br.weight)

    pl.loop(0, 2)(partial)

    @pl.when(is_last)
    def _():
        pl.loop(0, ready)(pair_sum)

    @pl.when(jnp.logical_not(is_last))
    def _():
        @pl.loop(0, micros)
        def _(m):
            @pl.when(helper(m) == section)
            def _():
                for br in branches:
                    gather_top(br, m)
                    lift_copy(br, m).start()

        pl.loop(0, micros)(pair_sum)

        @pl.loop(0, micros)
        def _(m):
            for br in branches:
                find_slope(br, m)

    @pl.loop(0, micros + 1)
    def _(step):
        @pl.when(step < micros)
        def _():
            spread(step)

        @pl.when(jnp.logical_and(is_last, step < micros - ready))
        def _():
            pair_sum(step + ready)

        @pl.when(step > 0)
        def _():
            descend(step - 1)

        @pl.when(jnp.logical_and(section < 2, step > 0))
        def _():
            hand_out(step - 1)

    @pl.when(section >= 2)
    def _():
        pl.loop(0, micros)(hand_out)

    @pl.loop(0, micros)
    def _(m):
        for br in branches:
            for k in range(1, parts):
                saved_copy(br, m, k).wait_send()
                out_copy(br, m, k).wait_send()
                out_copy(br, m, k).wait_recv()

            @pl.when(helper(m) == section)
            def _():
                for k in range(1, parts):
                    top_copy(br, m, k).wait_send()

                @pl.when(jnp.logical_not(is_last))
                def _():
                    lift_copy(br, m).wait_send()

            @pl.when(jnp.logical_not(is_first))
            def _():
                hop_copy(br, m).wait_send()

            pair_copy(br, m).wait_send()
            near_copy(br, m, 0).wait_send()
            for k in range(1, chips):
                chip_copy(br, m, k).wait_send()
                far_copy(br, m, k).wait_send()
                near_copy(br, m, k).wait_send()


def branch_call(sections, weights, saveds, tops):
    operands, outs, scratch = [], [], []
    for weight, saved, top in zip(weights, saveds, tops):
        rows, width = weight.shape
        micros, tokens = saved.shape[:2]
        parts = width // rows
        chips = parts // 2
        everyone = parts * tokens
        operands += [weight, saved, top]
        outs += [
            jax.ShapeDtypeStruct((parts, micros, tokens, rows), jnp.bfloat16),
            jax.ShapeDtypeStruct((micros, parts, tokens, rows), jnp.bfloat16),
            jax.ShapeDtypeStruct((micros, parts, everyone, rows), jnp.bfloat16),
        ]
        dma = pltpu.SemaphoreType.DMA
        scratch += [
            pltpu.VMEM((parts, rows, rows), jnp.bfloat16),
            pltpu.VMEM((parts, micros, tokens, rows), jnp.bfloat16),
            pltpu.VMEM((parts, micros, tokens, rows), jnp.bfloat16),
            pltpu.VMEM((micros, parts, tokens, rows), jnp.bfloat16),
            pltpu.VMEM((micros, parts, tokens, rows), jnp.bfloat16),
            dma((2, micros)),
            pltpu.VMEM((micros, parts, tokens, rows), jnp.bfloat16),
            pltpu.VMEM((micros, chips, everyone, rows), jnp.bfloat16),
            pltpu.VMEM((micros, chips, everyone, rows), jnp.bfloat16),
            pltpu.VMEM((micros, chips, everyone, rows), jnp.bfloat16),
            pltpu.VMEM((micros, max(chips - 1, 1), everyone, rows), jnp.bfloat16),
            pltpu.VMEM((micros, everyone, rows), jnp.float32),
            dma((2, micros, parts - 1)),
            dma((2, micros, parts - 1)),
            dma((2, micros)),
            dma((2, micros, max(chips - 1, 1))),
            dma((2, micros, chips)),
            dma((2, micros, max(chips - 1, 1))),
            dma((2, micros)),
            dma((2, micros, parts - 1)),
        ]
    vmem = pl.BlockSpec(memory_space=pltpu.VMEM)
    return pl.pallas_call(
        functools.partial(kernel, sections, parts, micros),
        out_shape=outs,
        in_specs=[vmem] * len(operands),
        out_specs=[vmem] * len(outs),
        scratch_shapes=scratch,
        compiler_params=pltpu.CompilerParams(
            collective_id=0, has_side_effects=True, vmem_limit_bytes=60 * 1024 * 1024
        ),
    )(*operands)


def finish_kernel(scale, *refs):
    outs, buffers, sems = refs[6:10], refs[10:14], refs[14]
    staged, in_sems = refs[15:21], refs[21]
    loads = [pltpu.make_async_copy(refs[i], staged[i], in_sems.at[i]) for i in range(6)]
    for i in (3, 4, 5, 0, 1, 2):
        loads[i].start()
    pending = []

    def flush(src, dst):
        copy = pltpu.make_async_copy(src, dst, sems.at[len(pending)])
        copy.start()
        pending.append(copy)

    for b in (1, 0):
        grads_in, columns, local = staged[3 * b : 3 * b + 3]
        for load in loads[3 * b : 3 * b + 3]:
            load.wait()
        grads, sums = outs[2 * b : 2 * b + 2]
        grad_buffer, sum_buffer = buffers[2 * b : 2 * b + 2]
        micros, parts, tokens, rows = columns.shape
        for part in range(parts):
            grad_buffer[:, :, part * rows : (part + 1) * rows] = grads_in[part]
        flush(grad_buffer, grads)
        lefts = [columns[:, group].reshape(micros * tokens, rows) for group in range(parts)]
        for part in range(parts):
            span = pl.ds(part * rows, rows)
            total = None
            for group in range(parts):
                right = local[:, part, group * tokens : (group + 1) * tokens]
                term = lax.dot_general(
                    lefts[group], right.reshape(micros * tokens, rows), (((0,), (0,)), ((), ())),
                    preferred_element_type=jnp.float32,
                )
                term = (term * scale).astype(jnp.bfloat16).astype(jnp.float32)
                total = term if total is None else total + term
            sum_buffer[:, part * rows : (part + 1) * rows] = total
            if rows % 128 == 0:
                flush(sum_buffer.at[:, span], sums.at[:, span])
        if rows % 128:
            flush(sum_buffer, sums)
    for copy in pending:
        copy.wait()


def finish(results, scale):
    outs, buffers = [], []
    for b in range(2):
        parts, micros, tokens, rows = results[3 * b].shape
        shapes = [((micros, tokens, parts * rows), jnp.bfloat16), ((rows, parts * rows), jnp.float32)]
        outs += [jax.ShapeDtypeStruct(*shape) for shape in shapes]
        buffers += [pltpu.VMEM(*shape) for shape in shapes]
    return pl.pallas_call(
        functools.partial(finish_kernel, scale),
        out_shape=outs,
        in_specs=[pl.BlockSpec(memory_space=pl.ANY)] * 6,
        out_specs=[pl.BlockSpec(memory_space=pl.ANY)] * 4,
        scratch_shapes=buffers
        + [pltpu.SemaphoreType.DMA((2 * parts + 4,))]
        + [pltpu.VMEM(result.shape, result.dtype) for result in results]
        + [pltpu.SemaphoreType.DMA((6,))],
        compiler_params=pltpu.CompilerParams(vmem_limit_bytes=63 * 1024 * 1024),
    )(*results)


def shards(vit_weight, t5_weight, vit_saved, t5_saved, vit_top_grad, t5_top_grad):
    sections = lax.axis_size("section")
    micros, tokens = t5_top_grad.shape[:2]
    scale = 1.0 / (micros * tokens)
    cut = 2 if tokens % 32 == 0 else 1

    def chunks(block):
        return block.reshape(micros * cut, tokens // cut, -1)

    results = branch_call(
        sections,
        [t5_weight[0], vit_weight[0]],
        [chunks(t5_saved[0]), chunks(vit_saved[0])],
        [chunks(t5_top_grad), chunks(vit_top_grad)],
    )
    t5_grads, t5_sum, vit_grads, vit_sum = finish(results, scale)
    return (
        vit_grads.reshape(vit_saved.shape),
        t5_grads.reshape(t5_saved.shape),
        vit_sum[None],
        t5_sum[None],
    )


def solution(mesh):
    placed = (
        P("section", "dp", None),
        P("section", "dp", None),
        P("section", None, "dp", None),
        P("section", None, "dp", None),
        P(None, "dp", None),
        P(None, "dp", None),
    )
    return jax.shard_map(
        shards,
        mesh=mesh,
        in_specs=placed,
        out_specs=(
            P("section", None, "dp", None),
            P("section", None, "dp", None),
            P("section", "dp", None),
            P("section", "dp", None),
        ),
        check_vma=False,
    )
```
